32 devices in a mesh: grp: 2 (over x), patch: 16 (over z, y, core).
Axes of the slice: x: 2, y: 2, z: 4, core: 2. Of those that a mesh axis runs over, the one named last changes fastest.
Arguments:
- features: bfloat16 [4, 16, 32, 640], P('grp', 'patch'), parts along dimension 0, may hold values from -6 to 6
- stale_conv_in: bfloat16 [4, 16, 32, 640], P('grp', 'patch'), parts along dimension 0, may hold values from -4.1875 to 4.1875
- stale_normed: bfloat16 [4, 16, 32, 640], P('grp', 'patch'), parts along dimension 0, may hold values from -6 to 6
- first_gain: float32 [640], replicated, may hold values from 0.1 to 1.9
- first_bias: float32 [640], replicated, may hold values from -1.8 to 1.8
- conv_weight: bfloat16 [3, 3, 640, 640], replicated, may hold values from -0.078125 to 0.078125
- conv_bias: float32 [640], replicated, may hold values from -1.8 to 1.8
- second_gain: float32 [640], replicated, may hold values from 0.1 to 1.9
- second_bias: float32 [640], replicated, may hold values from -1.8 to 1.8
- query_weight: bfloat16 [640, 640], replicated, may hold values from -6 to 6
- key_weight: bfloat16 [640, 640], replicated, may hold values from -6 to 6
- value_weight: bfloat16 [640, 640], replicated, may hold values from -0.25 to 0.25
- output_weight: bfloat16 [640, 640], replicated, may hold values from -0.25 to 0.25
- layer_gain: float32 [640], replicated, may hold values from 0.1 to 1.9
- cross_query: bfloat16 [640, 640], replicated, may hold values from -0.5 to 0.5
- cross_output: bfloat16 [640, 640], replicated, may hold values from -0.25 to 0.25
- text_keys: bfloat16 [4, 77, 640], P('grp'), parts along dimension 0, may hold values from -32 to 32
- text_values: bfloat16 [4, 77, 640], P('grp'), parts along dimension 0, may hold values from -6 to 6
Outputs:
- block_output: float32 [4, 16, 32, 640], P('grp', 'patch'), parts along dimension 0
The draws below stay inside these ranges and needn't reach their ends.
There are 2 independent parts, one for each index of `grp`. The reference program is written for one: setup_inputs(seed, part) draws one part's arguments, and reference() takes and returns one part's arrays. A program takes and returns all parts, laid end to end along the dimension named above; an argument that names none is the same for every part. Nothing has to cross between parts.
All inputs are finite; a program needn't handle non-finite values.
Results may differ from the reference program's by a relative error of at most 0.02.
The reference program's roundings to bfloat16 on the way count: a program that leaves them out, or rounds other values in their place, can miss the bound.
Values may be sent and summed in bfloat16 or wider, within the bound.
No kernel may reach another device: no remote copies, remote signals or barrier semaphores. Data moves between devices by JAX's collectives and lax.ppermute only.
A program may use at most 128 MiB of HBM per device.

```python
import jax
import jax.numpy as jnp
from jax import lax

C = 640
GROUPS = 32
HEADS = 10
HEAD_DIM = 64
CTX = 77
HALF = 32
ATT = 640
IMAGES = 2
PATCHES = 16


def draw_features(key, part):
    key_noise = jax.random.fold_in(key, 11)
    key_channel = jax.random.fold_in(key, 12)
    place = jnp.arange(PATCHES, dtype=jnp.float32) / (PATCHES - 1)
    row_scale = (0.6 + 1.2 * place)[None, :, None, None]
    channel_scale = jax.random.uniform(key_channel, (1, 1, 1, C), jnp.float32, 0.5, 1.5)
    noise = jax.random.normal(key_noise, (IMAGES, PATCHES, HALF, C), jnp.float32)
    values = noise * row_scale * channel_scale
    return jnp.clip(values, -6.0, 6.0).astype(jnp.bfloat16)


def drawn_weight(key, salt, spread):
    key_noise = jax.random.fold_in(key, salt)
    values = jax.random.normal(key_noise, (C, ATT), jnp.float32) * spread
    return jnp.clip(values, -6.0, 6.0).astype(jnp.bfloat16)


def draw_query_weight(key, part):
    return drawn_weight(key, 81, (C // 9) ** (-0.5))


def draw_key_weight(key, part):
    return drawn_weight(key, 82, C ** (-0.5))


def draw_text_keys(key, part):
    key_noise = jax.random.fold_in(key, 91)
    values = jnp.clip(jax.random.normal(key_noise, (IMAGES, CTX, ATT), jnp.float32), -6.0, 6.0)
    return jnp.clip(values, -32.0, 32.0).astype(jnp.bfloat16)


def levels(own_key, shape, cuts, smallest, high):
    gain, own = 1.0, jax.random.fold_in(own_key, 6)
    for axis_at, blocks in cuts:
        draws = jnp.exp(jax.random.uniform(jax.random.fold_in(own, axis_at), (blocks,), jnp.float32, smallest / len(cuts), high / len(cuts)))
        gain = gain * jnp.repeat(draws, shape[axis_at] // blocks).reshape([-1 if axis == axis_at else 1 for axis in range(len(shape))])
    return gain


def gaussian(own_key, dims, scale, reach, shards=(), kind=jnp.bfloat16):
    factor_of = levels(own_key, dims, shards, -0.22, 0.18) if shards else 1.0
    array = jax.random.normal(own_key, dims, jnp.float32) * scale * factor_of
    return jnp.minimum(jnp.maximum(array, -reach), reach).astype(kind)


def setup_inputs(seed: int = 0, part: int = 0) -> dict:
    splits = jax.random.split(jax.random.key(seed), 19)
    part_keys = jax.random.split(jax.random.fold_in(splits[18], part), 19)
    return {
        "features": draw_features(jax.random.fold_in(jax.random.fold_in(splits[18], part), 71), part),
        "stale_conv_in": gaussian(part_keys[1], (IMAGES, PATCHES, HALF, C), 0.7, 4.1875, ((1, 16),)),
        "stale_normed": gaussian(part_keys[2], (IMAGES, PATCHES, HALF, C), 1.0, 6.0, ((1, 16),)),
        "first_gain": jnp.clip(1.0 + 0.18 * jax.random.normal(splits[3], (C,), jnp.float32), 0.1, 1.9),
        "first_bias": gaussian(splits[4], (C,), 0.3, 1.8, (), jnp.float32),
        "conv_weight": gaussian(splits[5], (3, 3, C, C), (9 * C) ** -0.5, 0.078125),
        "conv_bias": gaussian(splits[6], (C,), 0.3, 1.8, (), jnp.float32),
        "second_gain": jnp.clip(1.0 + 0.18 * jax.random.normal(splits[7], (C,), jnp.float32), 0.1, 1.9),
        "second_bias": gaussian(splits[8], (C,), 0.3, 1.8, (), jnp.float32),
        "query_weight": draw_query_weight(jax.random.fold_in(splits[18], 71), part),
        "key_weight": draw_key_weight(jax.random.fold_in(splits[18], 71), part),
        "value_weight": gaussian(splits[11], (C, ATT), C ** -0.5, 0.25),
        "output_weight": gaussian(splits[12], (ATT, C), ATT ** -0.5, 0.25),
        "layer_gain": jnp.clip(1.0 + 0.18 * jax.random.normal(splits[13], (C,), jnp.float32), 0.1, 1.9),
        "cross_query": gaussian(splits[14], (C, ATT), (C // 4) ** -0.5, 0.5),
        "cross_output": gaussian(splits[15], (ATT, C), ATT ** -0.5, 0.25),
        "text_keys": draw_text_keys(jax.random.fold_in(jax.random.fold_in(splits[18], part), 71), part),
        "text_values": gaussian(part_keys[17], (IMAGES, CTX, ATT), 1.0, 6.0),
    }


EPSILON = 1e-05

def narrow_exact(values):
    return lax.optimization_barrier(values.astype(jnp.bfloat16)).astype(jnp.float32)

def project(values, weight):
    return jnp.dot(values, weight, preferred_element_type=jnp.float32).astype(jnp.bfloat16)

def group_norm(features, scale_vec, shift_vec):
    images, patches, columns, channels = features.shape
    grouped = features.astype(jnp.float32).reshape(images, patches, columns, GROUPS, channels // GROUPS)
    group_mean = lax.optimization_barrier(jnp.mean(grouped, axis=(1, 2, 4), keepdims=True))
    group_var = lax.optimization_barrier(jnp.mean(jnp.square(grouped - group_mean), axis=(1, 2, 4), keepdims=True))
    normed = ((grouped - group_mean) * lax.rsqrt(group_var + EPSILON)).reshape(features.shape)
    return normed * scale_vec + shift_vec

def layer_norm(values, scale_vec):
    layer_mean = lax.optimization_barrier(jnp.mean(values, axis=-1, keepdims=True))
    centred = values - layer_mean
    layer_var = lax.optimization_barrier(jnp.mean(centred * centred, axis=-1, keepdims=True))
    return centred * lax.rsqrt(layer_var + EPSILON) * scale_vec

def patch_conv(fresh, stale, conv_weight):
    images = fresh.shape[0]
    row_count = PATCHES // 2
    image = stale.reshape(images, row_count, 2 * HALF, C)
    padded = jnp.pad(image, ((0, 0), (1, 1), (1, 1), (0, 0)))
    halves = []
    for half_side in range(2):
        columns_cut = padded[:, :, half_side * HALF:half_side * HALF + HALF + 2]
        halves.append(jnp.stack([columns_cut[:, offset:offset + row_count] for offset in range(3)], axis=2))
    windows = jnp.stack(halves, axis=2)
    centre = fresh.reshape(images, row_count, 2, HALF, C)
    windows = windows.at[:, :, :, 1, 1:HALF + 1].set(centre)
    total = jnp.zeros((images * row_count * 2 * HALF, C), jnp.float32)
    for offset_row in range(3):
        for offset_col in range(3):
            tap = windows[:, :, :, offset_row, offset_col:offset_col + HALF].reshape(-1, C)
            total = total + jnp.dot(tap, conv_weight[offset_row, offset_col], preferred_element_type=jnp.float32)
    return total.reshape(images, PATCHES, HALF, C)

def softmax_apply(queries, keys, values, scale):
    scores = jnp.einsum('bqhd,bkhd->bhqk', queries.astype(jnp.float32), keys.astype(jnp.float32)) * scale
    maxima = lax.optimization_barrier(jnp.max(scores, axis=-1, keepdims=True))
    weights = jnp.exp(scores - maxima)
    totals = lax.optimization_barrier(jnp.sum(weights, axis=-1))
    numer = jnp.einsum('bhqk,bkhd->bhqd', narrow_exact(weights), values.astype(jnp.float32))
    return numer / totals[..., None]

def reference(features, stale_conv_in, stale_normed, first_gain, first_bias, conv_weight, conv_bias, second_gain, second_bias, query_weight, key_weight, value_weight, output_weight, layer_gain, cross_query, cross_output, text_keys, text_values):
    images = features.shape[0]
    scale = HEAD_DIM ** (-0.5)
    conv_input = jax.nn.silu(group_norm(features, first_gain, first_bias)).astype(jnp.bfloat16)
    conv_out = patch_conv(conv_input, stale_conv_in, conv_weight)
    hidden = features.astype(jnp.float32) + conv_out + conv_bias
    attn_input = group_norm(hidden, second_gain, second_bias).astype(jnp.bfloat16)
    flat_input = attn_input.reshape(-1, C)
    stale_flat = stale_normed.reshape(-1, C)
    shape_att = (images, PATCHES, HALF, ATT)
    queries = project(flat_input, query_weight).reshape(shape_att)
    fresh_keys = project(flat_input, key_weight).reshape(shape_att)
    fresh_values = project(flat_input, value_weight).reshape(shape_att)
    stale_keys = project(stale_flat, key_weight).reshape(shape_att)
    stale_values = project(stale_flat, value_weight).reshape(shape_att)

    def one_patch(position):
        patch_queries = lax.dynamic_slice_in_dim(queries, position, 1, 1).reshape(images, HALF, HEADS, HEAD_DIM)
        own_keys = lax.dynamic_slice_in_dim(fresh_keys, position, 1, 1)
        own_values = lax.dynamic_slice_in_dim(fresh_values, position, 1, 1)
        keys_all = lax.dynamic_update_slice_in_dim(stale_keys, own_keys, position, 1).reshape(images, PATCHES * HALF, HEADS, HEAD_DIM)
        values_all = lax.dynamic_update_slice_in_dim(stale_values, own_values, position, 1).reshape(images, PATCHES * HALF, HEADS, HEAD_DIM)
        result = softmax_apply(patch_queries, keys_all, values_all, scale)
        return result.transpose(0, 2, 1, 3).reshape(images, HALF, ATT).astype(jnp.bfloat16)
    attended = lax.map(one_patch, jnp.arange(PATCHES, dtype=jnp.int32)).transpose(1, 0, 2, 3)
    mixed = hidden.reshape(-1, C) + jnp.dot(attended.reshape(-1, ATT), output_weight, preferred_element_type=jnp.float32)
    layer_in = layer_norm(mixed, layer_gain).astype(jnp.bfloat16)
    cross_q = project(layer_in, cross_query).reshape(images, PATCHES * HALF, HEADS, HEAD_DIM)
    text_k = text_keys.reshape(images, CTX, HEADS, HEAD_DIM)
    text_v = text_values.reshape(images, CTX, HEADS, HEAD_DIM)
    cross_result = softmax_apply(cross_q, text_k, text_v, scale)
    cross_attn = cross_result.transpose(0, 2, 1, 3).reshape(-1, ATT).astype(jnp.bfloat16)
    block_output = mixed + jnp.dot(cross_attn, cross_output, preferred_element_type=jnp.float32)
    return block_output.reshape(images, PATCHES, HALF, C)
```

```python
import functools

import jax
import jax.numpy as jnp
from jax import lax
from jax.experimental import pallas as pl
from jax.experimental.pallas import tpu as pltpu
from jax.sharding import PartitionSpec as P

GROUPS = 32
HEADS = 10
HEAD_DIM = 64
EPSILON = 1e-05


VMEM = pl.BlockSpec(memory_space=pltpu.VMEM)
HBM = pl.BlockSpec(memory_space=pltpu.HBM)
F32 = jnp.float32
BF16 = jnp.bfloat16


def exchange(value, axis, apart):
    return lax.ppermute(value, axis, [(i, i ^ apart) for i in range(lax.axis_size(axis))])


def shifted(value, axis, steps):
    count = lax.axis_size(axis)
    initial, last = (max(0, -steps), min(count, count - steps))
    return lax.ppermute(value, axis, [(source, source + steps) for source in range(initial, last)])


def total_over(value, axis):
    apart = lax.axis_size(axis) // 2
    while apart:
        value = value + exchange(value, axis, apart)
        apart //= 2
    return value


def dot(a, b):
    return jnp.dot(a, b, preferred_element_type=F32)


def per_channel(sums, count):
    channels = sums.shape[-1]
    width = channels // GROUPS
    channel = lax.broadcasted_iota(jnp.int32, (channels, GROUPS), 0)
    low = lax.broadcasted_iota(jnp.int32, (channels, GROUPS), 1) * width
    member = jnp.where((channel >= low) & (channel < low + width), 1.0, 0.0)
    channel = lax.broadcasted_iota(jnp.int32, (GROUPS, channels), 1)
    low = lax.broadcasted_iota(jnp.int32, (GROUPS, channels), 0) * width
    spread = jnp.where((channel >= low) & (channel < low + width), 1.0, 0.0)
    exact = lax.Precision.HIGHEST
    grouped = jnp.dot(sums, member, preferred_element_type=F32, precision=exact)
    return jnp.dot(grouped, spread, preferred_element_type=F32, precision=exact) / count


def normalised(x, moments, image, images, gain, bias):
    mean = moments[image : image + 1]
    var = moments[images + image : images + image + 1] - mean * mean
    return (x - mean) * lax.rsqrt(var + EPSILON) * gain + bias


def stale_conv_body(taps_ref, weight_ref, out_ref):
    @pl.when(pl.program_id(0) == 0)
    def _():
        out_ref[...] = jnp.zeros_like(out_ref)

    out_ref[...] += dot(taps_ref[0], weight_ref[0, 0])


def stale_conv(taps, conv_weight):
    count, cells, channels = taps.shape
    return pl.pallas_call(
        stale_conv_body,
        grid=(count,),
        in_specs=[
            pl.BlockSpec((1, cells, channels), lambda t: (t, 0, 0)),
            pl.BlockSpec((1, 1, channels, channels), lambda t: (2 * (t // 3), t % 3, 0, 0)),
        ],
        out_specs=pl.BlockSpec((cells, channels), lambda t: (0, 0)),
        out_shape=jax.ShapeDtypeStruct((cells, channels), F32),
        cost_estimate=pl.CostEstimate(
            flops=2 * count * cells * channels * channels,
            transcendentals=0,
            bytes_accessed=2 * count * channels * channels,
        ),
        name="stale_conv",
    )(taps, conv_weight)


def centre_body(
    features_ref, sums_ref, gain_ref, bias_ref, left_ref, right_ref, stale_ref, conv_bias_ref,
    weight_ref, hidden_ref, out_sums_ref, weight_buf, sem, *, count,
):
    copy = pltpu.make_async_copy(weight_ref.at[1], weight_buf, sem.at[0])
    copy.start()
    images = left_ref.shape[0]
    cells = features_ref.shape[0]
    columns = cells // images
    moments = per_channel(sums_ref[...], count)
    taps = ([], [], [])
    for image in range(images):
        rows = slice(image * columns, (image + 1) * columns)
        x = features_ref[rows].astype(F32)
        x = normalised(x, moments, image, images, gain_ref[...], bias_ref[...])
        x = x * jax.nn.sigmoid(x)
        row = lax.broadcasted_iota(jnp.int32, x.shape, 0)
        taps[0].append(jnp.where(row == 0, left_ref[image : image + 1], pltpu.roll(x, 1, 0)))
        taps[1].append(x)
        taps[2].append(
            jnp.where(row == columns - 1, right_ref[image : image + 1], pltpu.roll(x, columns - 1, 0))
        )
    acc = features_ref[...].astype(F32) + stale_ref[...] + conv_bias_ref[...]
    copy.wait()
    for at, tap in enumerate(taps):
        acc = acc + dot(jnp.concatenate(tap, axis=0).astype(BF16), weight_buf[at])
    hidden_ref[...] = acc
    for image in range(images):
        x = acc[image * columns : (image + 1) * columns]
        out_sums_ref[image : image + 1] = jnp.sum(x, axis=0, keepdims=True)
        out_sums_ref[images + image : images + image + 1] = jnp.sum(x * x, axis=0, keepdims=True)


def centre(features, sums, gain, bias, left, right, stale, conv_bias, conv_weight, count):
    cells, channels = features.shape
    return pl.pallas_call(
        functools.partial(centre_body, count=count),
        in_specs=[VMEM] * 8 + [HBM],
        out_specs=[VMEM, VMEM],
        out_shape=[
            jax.ShapeDtypeStruct((cells, channels), F32),
            jax.ShapeDtypeStruct(sums.shape, F32),
        ],
        scratch_shapes=[
            pltpu.VMEM(conv_weight.shape[1:], BF16),
            pltpu.SemaphoreType.DMA((1,)),
        ],
        cost_estimate=pl.CostEstimate(
            flops=6 * cells * channels * channels,
            transcendentals=cells * channels,
            bytes_accessed=6 * channels * channels,
        ),
        name="centre_conv",
    )(features, sums, gain, bias, left, right, stale, conv_bias, conv_weight)


def attention(queries, key_of, value_of):
    columns, width = queries.shape
    parts = []
    for first in range(0, HEADS, 4):
        heads = min(4, HEADS - first)
        lanes = slice(first * HEAD_DIM, (first + heads) * HEAD_DIM)
        q = queries[:, lanes]
        lane = lax.broadcasted_iota(jnp.int32, q.shape, 1)
        inside = [(lane >= h * HEAD_DIM) & (lane < (h + 1) * HEAD_DIM) for h in range(heads)]
        stacked = jnp.concatenate([jnp.where(i, q, 0.0) for i in inside], axis=0).astype(BF16)
        scores = lax.dot_general(
            stacked, key_of(lanes), (((1,), (1,)), ((), ())), preferred_element_type=F32
        ) * (HEAD_DIM**-0.5)
        weights = jnp.exp(scores - jnp.max(scores, axis=-1, keepdims=True))
        total = jnp.sum(weights, axis=-1, keepdims=True)
        result = dot(weights.astype(BF16), value_of(lanes)) / total
        part = jnp.zeros_like(q)
        for h in range(heads):
            part = part + jnp.where(inside[h], result[h * columns : (h + 1) * columns], 0.0)
        parts.append(part)
    return jnp.concatenate(parts, axis=-1).astype(BF16)


def tail_body(
    hidden_ref, sums_ref, gain_ref, bias_ref, layer_gain_ref, text_keys_ref, text_values_ref,
    near_keys_ref, far_keys_ref, near_values_ref, far_values_ref,
    wq_ref, wk_ref, wv_ref, wo_ref, cq_ref, co_ref,
    out_ref, keys_buf, values_buf, weights_buf, sem, *, count,
):
    near = near_keys_ref.shape[0]
    moves = [
        (wq_ref, weights_buf.at[0]),
        (wk_ref, weights_buf.at[1]),
        (wv_ref, weights_buf.at[2]),
        (near_keys_ref.at[pl.ds(1, near - 1)], keys_buf.at[pl.ds(1, near - 1)]),
        (far_keys_ref, keys_buf.at[pl.ds(near, near)]),
        (near_values_ref.at[pl.ds(1, near - 1)], values_buf.at[pl.ds(1, near - 1)]),
        (far_values_ref, values_buf.at[pl.ds(near, near)]),
        (wo_ref, weights_buf.at[3]),
        (cq_ref, weights_buf.at[4]),
        (co_ref, weights_buf.at[5]),
    ]
    copies = [pltpu.make_async_copy(a, b, sem.at[i]) for i, (a, b) in enumerate(moves)]
    for copy in copies:
        copy.start()
    cells, channels = hidden_ref.shape
    images = text_keys_ref.shape[0]
    columns = cells // images
    patches = 2 * near
    moments = per_channel(sums_ref[...], count)
    rows = [slice(image * columns, (image + 1) * columns) for image in range(images)]
    x = jnp.concatenate(
        [
            normalised(hidden_ref[rows[i]], moments, i, images, gain_ref[...], bias_ref[...])
            for i in range(images)
        ],
        axis=0,
    ).astype(BF16)
    copies[0].wait()
    queries = dot(x, weights_buf[0]).astype(BF16).astype(F32)
    copies[1].wait()
    keys = dot(x, weights_buf[1]).astype(BF16)
    copies[2].wait()
    values = dot(x, weights_buf[2]).astype(BF16)
    for image in range(images):
        keys_buf[0, image] = keys[rows[image]]
        values_buf[0, image] = values[rows[image]]
    for copy in copies[3:7]:
        copy.wait()
    own = []
    for image in range(images):
        flat = lambda buf, lanes: buf[:, image, :, lanes].reshape(
            patches * columns, lanes.stop - lanes.start
        )
        own.append(
            attention(queries[rows[image]], lambda l: flat(keys_buf, l), lambda l: flat(values_buf, l))
        )
    copies[7].wait()
    mixed = hidden_ref[...] + dot(jnp.concatenate(own, axis=0), weights_buf[3])
    centred = mixed - jnp.mean(mixed, axis=-1, keepdims=True)
    var = jnp.mean(centred * centred, axis=-1, keepdims=True)
    layer_in = (centred * lax.rsqrt(var + EPSILON) * layer_gain_ref[...]).astype(BF16)
    copies[8].wait()
    cross_q = dot(layer_in, weights_buf[4]).astype(BF16).astype(F32)
    crossed = [
        attention(
            cross_q[rows[image]],
            lambda l: text_keys_ref[image, :, l],
            lambda l: text_values_ref[image, :, l],
        )
        for image in range(images)
    ]
    copies[9].wait()
    out_ref[...] = mixed + dot(jnp.concatenate(crossed, axis=0), weights_buf[5])


def tail(hidden, sums, gain, bias, layer_gain, text_keys, text_values, kept, weights, count):
    cells, channels = hidden.shape
    near, images, columns, width = kept[0].shape
    buffer = pltpu.VMEM((2 * near, images, columns, width), BF16)
    return pl.pallas_call(
        functools.partial(tail_body, count=count),
        in_specs=[VMEM] * 7 + [HBM] * 10,
        out_specs=VMEM,
        out_shape=jax.ShapeDtypeStruct((cells, channels), F32),
        scratch_shapes=[
            buffer,
            buffer,
            pltpu.VMEM((6, channels, width), BF16),
            pltpu.SemaphoreType.DMA((10,)),
        ],
        cost_estimate=pl.CostEstimate(
            flops=12 * cells * channels * width + 16 * near * columns * cells * width,
            transcendentals=2 * near * columns * cells * HEADS,
            bytes_accessed=12 * channels * width + 8 * near * images * columns * width,
        ),
        name="tail",
    )(hidden, sums, gain, bias, layer_gain, text_keys, text_values, *kept, *weights)


def on_device(
    features, stale_conv_in, stale_normed, first_gain, first_bias, conv_weight, conv_bias,
    second_gain, second_bias, query_weight, key_weight, value_weight, output_weight,
    layer_gain, cross_query, cross_output, text_keys, text_values,
):
    images, _, columns, channels = features.shape
    cells = images * columns
    patches = lax.axis_size("patch")
    count = patches * columns * (channels // GROUPS)
    wide = features.astype(F32)[:, 0]
    sums = jnp.concatenate([jnp.sum(wide, axis=1), jnp.sum(wide * wide, axis=1)], axis=0)
    sums = total_over(sums, "patch")

    stale = stale_conv_in[:, 0]
    right_side = lax.axis_index("patch") % 2 == 1
    edge = jnp.where(right_side, stale[:, 0], stale[:, -1])
    across = exchange(edge, "patch", 1)
    nothing = jnp.zeros_like(across)
    left = jnp.where(right_side, across, nothing)
    right = jnp.where(right_side, nothing, across)
    stale_wide = jnp.concatenate([left[:, None], stale, right[:, None]], axis=1)
    above = shifted(stale_wide, "patch", 2)
    below = shifted(stale_wide, "patch", -2)
    taps = jnp.stack(
        [row[:, at : at + columns].reshape(cells, channels) for row in (above, below) for at in range(3)]
    )
    partial = stale_conv(taps, conv_weight)

    held = stale_normed.reshape(1, images, columns, channels)
    apart = patches // 2
    while apart > 1:
        held = jnp.concatenate([held, exchange(held, "patch", apart)], axis=0)
        apart //= 2
    other = exchange(held, "patch", 1)
    kept = [
        dot(half.reshape(-1, channels), weight).astype(BF16).reshape(half.shape)
        for weight in (key_weight, value_weight)
        for half in (held, other)
    ]

    row = lambda v: v.reshape(1, channels)
    hidden, sums = centre(
        features.reshape(cells, channels), sums, row(first_gain), row(first_bias),
        left.astype(F32), right.astype(F32), partial, row(conv_bias), conv_weight, count,
    )
    sums = total_over(sums, "patch")
    out = tail(
        hidden, sums, row(second_gain), row(second_bias), row(layer_gain), text_keys, text_values,
        kept, (query_weight, key_weight, value_weight, output_weight, cross_query, cross_output), count,
    )
    return out.reshape(images, 1, columns, channels)


def solution(mesh):
    split = P("grp", "patch", None, None)
    in_specs = (split,) * 3 + (P(),) * 13 + (P("grp", None, None),) * 2
    return jax.shard_map(on_device, mesh=mesh, in_specs=in_specs, out_specs=split, check_vma=False)
```

```python
import functools

import jax
import jax.numpy as jnp
from jax import lax
from jax.experimental import pallas as pl
from jax.experimental.pallas import tpu as pltpu
from jax.sharding import PartitionSpec as P

GROUPS = 32
HEADS = 10
HEAD_DIM = 64
EPSILON = 1e-05


VMEM = pl.BlockSpec(memory_space=pltpu.VMEM)
HBM = pl.BlockSpec(memory_space=pltpu.HBM)
F32 = jnp.float32
BF16 = jnp.bfloat16


def exchange(value, axis, apart):
    return lax.ppermute(value, axis, [(i, i ^ apart) for i in range(lax.axis_size(axis))])


def shifted(value, axis, steps):
    count = lax.axis_size(axis)
    initial, last = (max(0, -steps), min(count, count - steps))
    return lax.ppermute(value, axis, [(source, source + steps) for source in range(initial, last)])


def total_over(value, axis):
    apart = lax.axis_size(axis) // 2
    while True:
        other = exchange(value, axis, apart)
        if apart == 1:
            return value, other
        value = value + other
        apart //= 2


def dot(a, b):
    return jnp.dot(a, b, preferred_element_type=F32)


def per_channel(sums, count):
    channels = sums.shape[-1]
    width = channels // GROUPS
    channel = lax.broadcasted_iota(jnp.int32, (channels, GROUPS), 0)
    low = lax.broadcasted_iota(jnp.int32, (channels, GROUPS), 1) * width
    member = jnp.where((channel >= low) & (channel < low + width), 1.0, 0.0)
    channel = lax.broadcasted_iota(jnp.int32, (GROUPS, channels), 1)
    low = lax.broadcasted_iota(jnp.int32, (GROUPS, channels), 0) * width
    spread = jnp.where((channel >= low) & (channel < low + width), 1.0, 0.0)
    exact = lax.Precision.HIGHEST
    grouped = jnp.dot(sums, member, preferred_element_type=F32, precision=exact)
    return jnp.dot(grouped, spread, preferred_element_type=F32, precision=exact) / count


def normalised(x, moments, image, images, gain, bias):
    mean = moments[image : image + 1]
    var = moments[images + image : images + image + 1] - mean * mean
    return (x - mean) * lax.rsqrt(var + EPSILON) * gain + bias


def three_taps(x, left, right):
    row = lax.broadcasted_iota(jnp.int32, x.shape, 0)
    last = x.shape[0] - 1
    return (
        jnp.where(row == 0, left, pltpu.roll(x, 1, 0)),
        x,
        jnp.where(row == last, right, pltpu.roll(x, last, 0)),
    )


def conv_body(
    features_ref, mine_ref, other_ref, gain_ref, bias_ref, above_ref, level_ref, below_ref,
    conv_bias_ref, weight_ref, hidden_ref, sums_ref, weight_buf, sem, *, count,
):
    order = [(row, column) for row in (0, 2, 1) for column in range(3)]
    copies = [
        pltpu.make_async_copy(weight_ref.at[i, j], weight_buf.at[i, j], sem.at[3 * i + j])
        for i, j in order
    ]
    for copy in copies:
        copy.start()
    images = above_ref.shape[0]
    cells, channels = features_ref.shape
    columns = cells // images
    moments = per_channel(mine_ref[...] + other_ref[...], count)
    gain, bias, conv_bias = [r[...].reshape(1, channels) for r in (gain_ref, bias_ref, conv_bias_ref)]
    taps = {at: [] for at in order}
    for image in range(images):
        x = features_ref[image * columns : (image + 1) * columns].astype(F32)
        x = normalised(x, moments, image, images, gain, bias)
        fresh = x * jax.nn.sigmoid(x)
        for i, ref in enumerate((above_ref, level_ref, below_ref)):
            held = ref[image].astype(F32)
            middle = fresh if i == 1 else held[:columns]
            edges = (held[columns : columns + 1], held[columns + 1 : columns + 2])
            for j, tap in enumerate(three_taps(middle, *edges)):
                taps[i, j].append(tap)
    acc = features_ref[...].astype(F32) + conv_bias
    for copy, at in zip(copies, order):
        tap = jnp.concatenate(taps[at], axis=0).astype(BF16)
        copy.wait()
        acc = acc + dot(tap, weight_buf[at[0], at[1]])
    hidden_ref[...] = acc
    for image in range(images):
        x = acc[image * columns : (image + 1) * columns]
        sums_ref[image : image + 1] = jnp.sum(x, axis=0, keepdims=True)
        sums_ref[images + image : images + image + 1] = jnp.sum(x * x, axis=0, keepdims=True)


def conv(features, sums, gain, bias, above, level, below, conv_bias, conv_weight, count):
    cells, channels = features.shape
    return pl.pallas_call(
        functools.partial(conv_body, count=count),
        in_specs=[VMEM] * 9 + [HBM],
        out_specs=[VMEM, VMEM],
        out_shape=[
            jax.ShapeDtypeStruct((cells, channels), F32),
            jax.ShapeDtypeStruct(sums[0].shape, F32),
        ],
        scratch_shapes=[
            pltpu.VMEM(conv_weight.shape, BF16),
            pltpu.SemaphoreType.DMA((9,)),
        ],
        cost_estimate=pl.CostEstimate(
            flops=18 * cells * channels * channels,
            transcendentals=cells * channels,
            bytes_accessed=18 * channels * channels,
        ),
        name="conv",
    )(features, *sums, gain, bias, above, level, below, conv_bias, conv_weight)


def attention(queries, key_of, value_of):
    columns, _ = queries.shape
    parts = []
    for first in range(0, HEADS, 4):
        heads = min(4, HEADS - first)
        lanes = slice(first * HEAD_DIM, (first + heads) * HEAD_DIM)
        q = queries[:, lanes]
        lane = lax.broadcasted_iota(jnp.int32, q.shape, 1)
        inside = [(lane >= h * HEAD_DIM) & (lane < (h + 1) * HEAD_DIM) for h in range(heads)]
        stacked = jnp.concatenate([jnp.where(i, q, 0.0) for i in inside], axis=0).astype(BF16)
        scores = lax.dot_general(
            stacked, key_of(lanes), (((1,), (1,)), ((), ())), preferred_element_type=F32
        ) * (HEAD_DIM**-0.5)
        weights = jnp.exp(scores - jnp.max(scores, axis=-1, keepdims=True))
        total = jnp.sum(weights, axis=-1, keepdims=True)
        result = dot(weights.astype(BF16), value_of(lanes)) / total
        part = jnp.zeros_like(q)
        for h in range(heads):
            part = part + jnp.where(inside[h], result[h * columns : (h + 1) * columns], 0.0)
        parts.append(part)
    return jnp.concatenate(parts, axis=-1).astype(BF16)


def tail_body(
    hidden_ref, mine_ref, other_ref, gain_ref, bias_ref, layer_gain_ref, text_keys_ref, text_values_ref,
    near_keys_ref, far_keys_ref, near_values_ref, far_values_ref,
    wq_ref, wk_ref, wv_ref, wo_ref, cq_ref, co_ref,
    out_ref, keys_buf, values_buf, weights_buf, sem, *, count,
):
    near = near_keys_ref.shape[0]
    moves = [
        (wq_ref, weights_buf.at[0]),
        (wk_ref, weights_buf.at[1]),
        (wv_ref, weights_buf.at[2]),
        (near_keys_ref.at[pl.ds(1, near - 1)], keys_buf.at[pl.ds(1, near - 1)]),
        (far_keys_ref, keys_buf.at[pl.ds(near, near)]),
        (near_values_ref.at[pl.ds(1, near - 1)], values_buf.at[pl.ds(1, near - 1)]),
        (far_values_ref, values_buf.at[pl.ds(near, near)]),
        (wo_ref, weights_buf.at[3]),
        (cq_ref, weights_buf.at[4]),
        (co_ref, weights_buf.at[5]),
    ]
    copies = [pltpu.make_async_copy(a, b, sem.at[i]) for i, (a, b) in enumerate(moves)]
    for copy in copies:
        copy.start()
    cells, channels = hidden_ref.shape
    images = text_keys_ref.shape[0]
    columns = cells // images
    patches = 2 * near
    moments = per_channel(mine_ref[...] + other_ref[...], count)
    gain, bias, layer_gain = [r[...].reshape(1, channels) for r in (gain_ref, bias_ref, layer_gain_ref)]
    rows = [slice(image * columns, (image + 1) * columns) for image in range(images)]
    x = jnp.concatenate(
        [
            normalised(hidden_ref[rows[i]], moments, i, images, gain, bias)
            for i in range(images)
        ],
        axis=0,
    ).astype(BF16)
    copies[0].wait()
    queries = dot(x, weights_buf[0]).astype(BF16).astype(F32)
    copies[1].wait()
    keys = dot(x, weights_buf[1]).astype(BF16)
    copies[2].wait()
    values = dot(x, weights_buf[2]).astype(BF16)
    for image in range(images):
        keys_buf[0, image] = keys[rows[image]]
        values_buf[0, image] = values[rows[image]]
    for copy in copies[3:7]:
        copy.wait()
    own = []
    for image in range(images):
        flat = lambda buf, lanes: buf[:, image, :, lanes].reshape(
            patches * columns, lanes.stop - lanes.start
        )
        own.append(
            attention(queries[rows[image]], lambda l: flat(keys_buf, l), lambda l: flat(values_buf, l))
        )
    copies[7].wait()
    mixed = hidden_ref[...] + dot(jnp.concatenate(own, axis=0), weights_buf[3])
    centred = mixed - jnp.mean(mixed, axis=-1, keepdims=True)
    var = jnp.mean(centred * centred, axis=-1, keepdims=True)
    layer_in = (centred * lax.rsqrt(var + EPSILON) * layer_gain).astype(BF16)
    copies[8].wait()
    cross_q = dot(layer_in, weights_buf[4]).astype(BF16).astype(F32)
    crossed = [
        attention(
            cross_q[rows[image]],
            lambda l: text_keys_ref[image, :, l],
            lambda l: text_values_ref[image, :, l],
        )
        for image in range(images)
    ]
    copies[9].wait()
    out_ref[...] = mixed + dot(jnp.concatenate(crossed, axis=0), weights_buf[5])


def tail(hidden, sums, gain, bias, layer_gain, text_keys, text_values, kept, weights, count):
    cells, channels = hidden.shape
    near, images, columns, width = kept[0].shape
    buffer = pltpu.VMEM((2 * near, images, columns, width), BF16)
    return pl.pallas_call(
        functools.partial(tail_body, count=count),
        in_specs=[VMEM] * 8 + [HBM] * 10,
        out_specs=VMEM,
        out_shape=jax.ShapeDtypeStruct((cells, channels), F32),
        scratch_shapes=[
            buffer,
            buffer,
            pltpu.VMEM((6, channels, width), BF16),
            pltpu.SemaphoreType.DMA((10,)),
        ],
        cost_estimate=pl.CostEstimate(
            flops=12 * cells * channels * width + 16 * near * columns * cells * width,
            transcendentals=2 * near * columns * cells * HEADS,
            bytes_accessed=12 * channels * width + 8 * near * images * columns * width,
        ),
        name="tail",
    )(hidden, *sums, gain, bias, layer_gain, text_keys, text_values, *kept, *weights)


def on_device(
    features, stale_conv_in, stale_normed, first_gain, first_bias, conv_weight, conv_bias,
    second_gain, second_bias, query_weight, key_weight, value_weight, output_weight,
    layer_gain, cross_query, cross_output, text_keys, text_values,
):
    images, _, columns, channels = features.shape
    cells = images * columns
    patches = lax.axis_size("patch")
    count = patches * columns * (channels // GROUPS)
    wide = features.astype(F32)[:, 0]
    sums = jnp.concatenate([jnp.sum(wide, axis=1), jnp.sum(wide * wide, axis=1)], axis=0)
    sums = total_over(sums, "patch")

    stale = stale_conv_in[:, 0]
    right_side = lax.axis_index("patch") % 2 == 1
    across = exchange(stale, "patch", 1)
    left = jnp.where(right_side, across[:, -1:], 0)
    right = jnp.where(right_side, 0, across[:, :1])
    level = jnp.concatenate([stale, left, right, jnp.zeros_like(stale[:, :6])], axis=1)
    above = shifted(level, "patch", 2)
    below = shifted(level, "patch", -2)

    held = stale_normed.reshape(1, images, columns, channels)
    apart = patches // 2
    while apart:
        other = exchange(held, "patch", apart)
        if apart > 1:
            held = jnp.concatenate([held, other], axis=0)
        apart //= 2
    kept = []
    for weight in (key_weight, value_weight):
        for part in (held, other):
            kept.append(dot(part.reshape(-1, channels), weight).astype(BF16).reshape(part.shape))

    hidden, sums = conv(
        features.reshape(cells, channels), sums, first_gain, first_bias,
        above, level, below, conv_bias, conv_weight, count,
    )
    sums = total_over(sums, "patch")
    out = tail(
        hidden, sums, second_gain, second_bias, layer_gain, text_keys, text_values,
        kept, (query_weight, key_weight, value_weight, output_weight, cross_query, cross_output), count,
    )
    return out.reshape(images, 1, columns, channels)


def solution(mesh):
    split = P("grp", "patch", None, None)
    in_specs = (split,) * 3 + (P(),) * 13 + (P("grp", None, None),) * 2
    return jax.shard_map(on_device, mesh=mesh, in_specs=in_specs, out_specs=split, check_vma=False)
```

```python
import functools

import jax
import jax.numpy as jnp
from jax import lax
from jax.experimental import pallas as pl
from jax.experimental.pallas import tpu as pltpu
from jax.sharding import PartitionSpec as P

GROUPS = 32
HEADS = 10
HEAD_DIM = 64
EPSILON = 1e-05


VMEM = pl.BlockSpec(memory_space=pltpu.VMEM)
HBM = pl.BlockSpec(memory_space=pltpu.HBM)
F32 = jnp.float32
BF16 = jnp.bfloat16


def exchange(value, axis, apart):
    return lax.ppermute(value, axis, [(i, i ^ apart) for i in range(lax.axis_size(axis))])


def shifted(value, axis, steps):
    count = lax.axis_size(axis)
    initial, last = (max(0, -steps), min(count, count - steps))
    return lax.ppermute(value, axis, [(source, source + steps) for source in range(initial, last)])


def total_over(value, axis):
    apart = lax.axis_size(axis) // 2
    while True:
        other = exchange(value, axis, apart)
        if apart == 1:
            return value, other
        value = value + other
        apart //= 2


def dot(a, b):
    return jnp.dot(a, b, preferred_element_type=F32)


def per_channel(sums, count):
    channels = sums.shape[-1]
    width = channels // GROUPS
    channel = lax.broadcasted_iota(jnp.int32, (channels, GROUPS), 0)
    low = lax.broadcasted_iota(jnp.int32, (channels, GROUPS), 1) * width
    member = jnp.where((channel >= low) & (channel < low + width), 1.0, 0.0).astype(BF16)
    channel = lax.broadcasted_iota(jnp.int32, (GROUPS, channels), 1)
    low = lax.broadcasted_iota(jnp.int32, (GROUPS, channels), 0) * width
    spread = jnp.where((channel >= low) & (channel < low + width), 1.0, 0.0).astype(BF16)
    return exact_dot(exact_dot(sums, member), spread) / count


def exact_dot(a, ones):
    high = a.astype(BF16)
    rest = a - high.astype(F32)
    middle = rest.astype(BF16)
    low = (rest - middle.astype(F32)).astype(BF16)
    return dot(high, ones) + dot(middle, ones) + dot(low, ones)


def normalised(x, moments, image, images, gain, bias):
    mean = moments[image : image + 1]
    var = moments[images + image : images + image + 1] - mean * mean
    return (x - mean) * lax.rsqrt(var + EPSILON) * gain + bias


def three_taps(x, left, right):
    row = lax.broadcasted_iota(jnp.int32, x.shape, 0)
    last = x.shape[0] - 1
    return (
        jnp.where(row == 0, left, pltpu.roll(x, 1, 0)),
        x,
        jnp.where(row == last, right, pltpu.roll(x, last, 0)),
    )


def conv_body(
    features_ref, mine_ref, other_ref, gain_ref, bias_ref, above_ref, level_ref, below_ref,
    conv_bias_ref, weight_ref, hidden_ref, sums_ref, weight_buf, sem, *, count,
):
    order = (0, 2, 1)
    copies = [pltpu.make_async_copy(weight_ref.at[i], weight_buf.at[i], sem.at[i]) for i in order]
    for copy in copies:
        copy.start()
    images = above_ref.shape[0]
    cells, channels = features_ref.shape
    columns = cells // images
    moments = per_channel(mine_ref[...] + other_ref[...], count)
    gain, bias, conv_bias = [r[...].reshape(1, channels) for r in (gain_ref, bias_ref, conv_bias_ref)]
    taps = ([], [], [])
    for image in range(images):
        x = features_ref[image * columns : (image + 1) * columns].astype(F32)
        x = normalised(x, moments, image, images, gain, bias)
        fresh = x * jax.nn.sigmoid(x)
        for i, ref in enumerate((above_ref, level_ref, below_ref)):
            held = ref[image].astype(F32)
            middle = fresh if i == 1 else held[:columns]
            edges = (held[columns : columns + 1], held[columns + 1 : columns + 2])
            row_taps = three_taps(middle, *edges)
            taps[i].append(jnp.concatenate([t.astype(BF16) for t in row_taps], axis=1))
    acc = features_ref[...].astype(F32) + conv_bias
    for i, copy in zip(order, copies):
        copy.wait()
        tap = jnp.concatenate(taps[i], axis=0)
        acc = acc + dot(tap, weight_buf[i].reshape(3 * channels, channels))
    hidden_ref[...] = acc
    for image in range(images):
        x = acc[image * columns : (image + 1) * columns]
        sums_ref[image : image + 1] = jnp.sum(x, axis=0, keepdims=True)
        sums_ref[images + image : images + image + 1] = jnp.sum(x * x, axis=0, keepdims=True)


def conv(features, sums, gain, bias, above, level, below, conv_bias, conv_weight, count):
    cells, channels = features.shape
    return pl.pallas_call(
        functools.partial(conv_body, count=count),
        in_specs=[VMEM] * 9 + [HBM],
        out_specs=[VMEM, VMEM],
        out_shape=[
            jax.ShapeDtypeStruct((cells, channels), F32),
            jax.ShapeDtypeStruct(sums[0].shape, F32),
        ],
        scratch_shapes=[
            pltpu.VMEM(conv_weight.shape, BF16),
            pltpu.SemaphoreType.DMA((3,)),
        ],
        cost_estimate=pl.CostEstimate(
            flops=18 * cells * channels * channels,
            transcendentals=cells * channels,
            bytes_accessed=18 * channels * channels,
        ),
        name="conv",
    )(features, *sums, gain, bias, above, level, below, conv_bias, conv_weight)


def attention(queries, key_of, value_of):
    columns, _ = queries.shape
    parts = []
    for first in range(0, HEADS, 4):
        heads = min(4, HEADS - first)
        lanes = slice(first * HEAD_DIM, (first + heads) * HEAD_DIM)
        q = queries[:, lanes]
        lane = lax.broadcasted_iota(jnp.int32, q.shape, 1)
        inside = [(lane >= h * HEAD_DIM) & (lane < (h + 1) * HEAD_DIM) for h in range(heads)]
        stacked = jnp.concatenate([jnp.where(i, q, 0.0) for i in inside], axis=0).astype(BF16)
        scores = lax.dot_general(
            stacked, key_of(lanes), (((1,), (1,)), ((), ())), preferred_element_type=F32
        ) * (HEAD_DIM**-0.5)
        weights = jnp.exp(scores - jnp.max(scores, axis=-1, keepdims=True))
        total = jnp.sum(weights, axis=-1, keepdims=True)
        result = dot(weights.astype(BF16), value_of(lanes)) / total
        part = jnp.zeros_like(q)
        for h in range(heads):
            part = part + jnp.where(inside[h], result[h * columns : (h + 1) * columns], 0.0)
        parts.append(part)
    return jnp.concatenate(parts, axis=-1).astype(BF16)


def tail_body(
    hidden_ref, mine_ref, other_ref, gain_ref, bias_ref, layer_gain_ref, text_keys_ref, text_values_ref,
    near_keys_ref, far_keys_ref, near_values_ref, far_values_ref,
    wq_ref, wk_ref, wv_ref, wo_ref, cq_ref, co_ref,
    out_ref, keys_buf, values_buf, weights_buf, sem, *, count,
):
    near = near_keys_ref.shape[0]
    moves = [
        (wq_ref, weights_buf.at[0]),
        (wk_ref, weights_buf.at[1]),
        (wv_ref, weights_buf.at[2]),
        (near_keys_ref.at[pl.ds(1, near - 1)], keys_buf.at[pl.ds(1, near - 1)]),
        (far_keys_ref, keys_buf.at[pl.ds(near, near)]),
        (near_values_ref.at[pl.ds(1, near - 1)], values_buf.at[pl.ds(1, near - 1)]),
        (far_values_ref, values_buf.at[pl.ds(near, near)]),
        (wo_ref, weights_buf.at[3]),
        (cq_ref, weights_buf.at[4]),
        (co_ref, weights_buf.at[5]),
    ]
    copies = [pltpu.make_async_copy(a, b, sem.at[i]) for i, (a, b) in enumerate(moves)]
    for copy in copies:
        copy.start()
    cells, channels = hidden_ref.shape
    images = text_keys_ref.shape[0]
    columns = cells // images
    patches = 2 * near
    moments = per_channel(mine_ref[...] + other_ref[...], count)
    gain, bias, layer_gain = [r[...].reshape(1, channels) for r in (gain_ref, bias_ref, layer_gain_ref)]
    rows = [slice(image * columns, (image + 1) * columns) for image in range(images)]
    x = jnp.concatenate(
        [
            normalised(hidden_ref[rows[i]], moments, i, images, gain, bias)
            for i in range(images)
        ],
        axis=0,
    ).astype(BF16)
    copies[0].wait()
    queries = dot(x, weights_buf[0]).astype(BF16).astype(F32)
    copies[1].wait()
    keys = dot(x, weights_buf[1]).astype(BF16)
    copies[2].wait()
    values = dot(x, weights_buf[2]).astype(BF16)
    for image in range(images):
        keys_buf[0, image] = keys[rows[image]]
        values_buf[0, image] = values[rows[image]]
    for copy in copies[3:7]:
        copy.wait()
    own = []
    for image in range(images):
        flat = lambda buf, lanes: buf[:, image, :, lanes].reshape(
            patches * columns, lanes.stop - lanes.start
        )
        own.append(
            attention(queries[rows[image]], lambda l: flat(keys_buf, l), lambda l: flat(values_buf, l))
        )
    copies[7].wait()
    mixed = hidden_ref[...] + dot(jnp.concatenate(own, axis=0), weights_buf[3])
    centred = mixed - jnp.mean(mixed, axis=-1, keepdims=True)
    var = jnp.mean(centred * centred, axis=-1, keepdims=True)
    layer_in = (centred * lax.rsqrt(var + EPSILON) * layer_gain).astype(BF16)
    copies[8].wait()
    cross_q = dot(layer_in, weights_buf[4]).astype(BF16).astype(F32)
    crossed = [
        attention(
            cross_q[rows[image]],
            lambda l: text_keys_ref[image, :, l],
            lambda l: text_values_ref[image, :, l],
        )
        for image in range(images)
    ]
    copies[9].wait()
    out_ref[...] = mixed + dot(jnp.concatenate(crossed, axis=0), weights_buf[5])


def tail(hidden, sums, gain, bias, layer_gain, text_keys, text_values, kept, weights, count):
    cells, channels = hidden.shape
    near, images, columns, width = kept[0].shape
    buffer = pltpu.VMEM((2 * near, images, columns, width), BF16)
    return pl.pallas_call(
        functools.partial(tail_body, count=count),
        in_specs=[VMEM] * 8 + [HBM] * 10,
        out_specs=VMEM,
        out_shape=jax.ShapeDtypeStruct((cells, channels), F32),
        scratch_shapes=[
            buffer,
            buffer,
            pltpu.VMEM((6, channels, width), BF16),
            pltpu.SemaphoreType.DMA((10,)),
        ],
        cost_estimate=pl.CostEstimate(
            flops=12 * cells * channels * width + 16 * near * columns * cells * width,
            transcendentals=2 * near * columns * cells * HEADS,
            bytes_accessed=12 * channels * width + 8 * near * images * columns * width,
        ),
        name="tail",
    )(hidden, *sums, gain, bias, layer_gain, text_keys, text_values, *kept, *weights)


def on_device(
    features, stale_conv_in, stale_normed, first_gain, first_bias, conv_weight, conv_bias,
    second_gain, second_bias, query_weight, key_weight, value_weight, output_weight,
    layer_gain, cross_query, cross_output, text_keys, text_values,
):
    images, _, columns, channels = features.shape
    cells = images * columns
    patches = lax.axis_size("patch")
    count = patches * columns * (channels // GROUPS)
    wide = features.astype(F32)[:, 0]
    sums = jnp.concatenate([jnp.sum(wide, axis=1), jnp.sum(wide * wide, axis=1)], axis=0)
    sums = total_over(sums, "patch")

    stale = stale_conv_in[:, 0]
    right_side = lax.axis_index("patch") % 2 == 1
    across = exchange(stale, "patch", 1)
    left = jnp.where(right_side, across[:, -1:], 0)
    right = jnp.where(right_side, 0, across[:, :1])
    level = jnp.concatenate([stale, left, right, jnp.zeros_like(stale[:, :6])], axis=1)
    above = shifted(level, "patch", 2)
    below = shifted(level, "patch", -2)

    held = stale_normed.reshape(1, images, columns, channels)
    apart = patches // 2
    while apart:
        other = exchange(held, "patch", apart)
        if apart > 1:
            held = jnp.concatenate([held, other], axis=0)
        apart //= 2
    kept = []
    for weight in (key_weight, value_weight):
        for part in (held, other):
            kept.append(dot(part.reshape(-1, channels), weight).astype(BF16).reshape(part.shape))

    hidden, sums = conv(
        features.reshape(cells, channels), sums, first_gain, first_bias,
        above, level, below, conv_bias, conv_weight, count,
    )
    sums = total_over(sums, "patch")
    out = tail(
        hidden, sums, second_gain, second_bias, layer_gain, text_keys, text_values,
        kept, (query_weight, key_weight, value_weight, output_weight, cross_query, cross_output), count,
    )
    return out.reshape(images, 1, columns, channels)


def solution(mesh):
    split = P("grp", "patch", None, None)
    in_specs = (split,) * 3 + (P(),) * 13 + (P("grp", None, None),) * 2
    return jax.shard_map(on_device, mesh=mesh, in_specs=in_specs, out_specs=split, check_vma=False)
```

```python
import functools

import jax
import jax.numpy as jnp
from jax import lax
from jax.experimental import pallas as pl
from jax.experimental.pallas import tpu as pltpu
from jax.sharding import PartitionSpec as P

GROUPS = 32
HEADS = 10
HEAD_DIM = 64
EPSILON = 1e-05


VMEM = pl.BlockSpec(memory_space=pltpu.VMEM)
HBM = pl.BlockSpec(memory_space=pltpu.HBM)
F32 = jnp.float32
BF16 = jnp.bfloat16


def exchange(value, axis, apart):
    return lax.ppermute(value, axis, [(i, i ^ apart) for i in range(lax.axis_size(axis))])


def shifted(value, axis, steps):
    count = lax.axis_size(axis)
    initial, last = (max(0, -steps), min(count, count - steps))
    return lax.ppermute(value, axis, [(source, source + steps) for source in range(initial, last)])


def total_over(value, axis):
    apart = lax.axis_size(axis) // 2
    while True:
        other = exchange(value, axis, apart)
        if apart == 1:
            return value, other
        value = value + other
        apart //= 2


def dot(a, b):
    return jnp.dot(a, b, preferred_element_type=F32)


def per_channel(sums, count):
    channels = sums.shape[-1]
    width = channels // GROUPS
    channel = lax.broadcasted_iota(jnp.int32, (channels, GROUPS), 0)
    low = lax.broadcasted_iota(jnp.int32, (channels, GROUPS), 1) * width
    member = jnp.where((channel >= low) & (channel < low + width), 1.0, 0.0).astype(BF16)
    channel = lax.broadcasted_iota(jnp.int32, (GROUPS, channels), 1)
    low = lax.broadcasted_iota(jnp.int32, (GROUPS, channels), 0) * width
    spread = jnp.where((channel >= low) & (channel < low + width), 1.0, 0.0).astype(BF16)
    return exact_dot(exact_dot(sums, member), spread) / count


def exact_dot(a, ones):
    high = a.astype(BF16)
    rest = a - high.astype(F32)
    middle = rest.astype(BF16)
    low = (rest - middle.astype(F32)).astype(BF16)
    return dot(high, ones) + dot(middle, ones) + dot(low, ones)


def normalised(x, moments, image, images, gain, bias):
    mean = moments[image : image + 1]
    var = moments[images + image : images + image + 1] - mean * mean
    return (x - mean) * lax.rsqrt(var + EPSILON) * gain + bias


def three_taps(x, left, right):
    row = lax.broadcasted_iota(jnp.int32, x.shape, 0)
    last = x.shape[0] - 1
    return (
        jnp.where(row == 0, left, pltpu.roll(x, 1, 0)),
        x,
        jnp.where(row == last, right, pltpu.roll(x, last, 0)),
    )


def long_taps(middle, left, right):
    return jnp.concatenate([t.astype(BF16) for t in three_taps(middle, left, right)], axis=1)


def stale_body(above_ref, below_ref, weight_ref, out_ref, weight_buf, sem):
    copies = [pltpu.make_async_copy(weight_ref.at[2 * i], weight_buf.at[i], sem.at[i]) for i in range(2)]
    for copy in copies:
        copy.start()
    images = above_ref.shape[0]
    cells, channels = out_ref.shape
    columns = cells // images
    acc = None
    for i, ref in enumerate((above_ref, below_ref)):
        held = [ref[image].astype(F32) for image in range(images)]
        tap = jnp.concatenate(
            [long_taps(h[:columns], h[columns : columns + 1], h[columns + 1 : columns + 2]) for h in held],
            axis=0,
        )
        copies[i].wait()
        part = dot(tap, weight_buf[i].reshape(3 * channels, channels))
        acc = part if acc is None else acc + part
    out_ref[...] = acc


def stale_conv(above, below, conv_weight, cells):
    channels = conv_weight.shape[-1]
    return pl.pallas_call(
        stale_body,
        in_specs=[VMEM, VMEM, HBM],
        out_specs=VMEM,
        out_shape=jax.ShapeDtypeStruct((cells, channels), F32),
        scratch_shapes=[
            pltpu.VMEM((2,) + conv_weight.shape[1:], BF16),
            pltpu.SemaphoreType.DMA((2,)),
        ],
        cost_estimate=pl.CostEstimate(
            flops=12 * cells * channels * channels,
            transcendentals=0,
            bytes_accessed=12 * channels * channels,
        ),
        name="stale_conv",
    )(above, below, conv_weight)


def conv_body(
    features_ref, mine_ref, other_ref, gain_ref, bias_ref, level_ref, stale_ref,
    conv_bias_ref, weight_ref, hidden_ref, sums_ref, weight_buf, sem, *, count,
):
    copy = pltpu.make_async_copy(weight_ref.at[1], weight_buf, sem.at[0])
    copy.start()
    images = level_ref.shape[0]
    cells, channels = features_ref.shape
    columns = cells // images
    moments = per_channel(mine_ref[...] + other_ref[...], count)
    gain, bias, conv_bias = [r[...].reshape(1, channels) for r in (gain_ref, bias_ref, conv_bias_ref)]
    taps = []
    for image in range(images):
        x = features_ref[image * columns : (image + 1) * columns].astype(F32)
        x = normalised(x, moments, image, images, gain, bias)
        held = level_ref[image].astype(F32)
        taps.append(
            long_taps(x * jax.nn.sigmoid(x), held[columns : columns + 1], held[columns + 1 : columns + 2])
        )
    acc = features_ref[...].astype(F32) + conv_bias + stale_ref[...]
    copy.wait()
    acc = acc + dot(jnp.concatenate(taps, axis=0), weight_buf[...].reshape(3 * channels, channels))
    hidden_ref[...] = acc
    for image in range(images):
        x = acc[image * columns : (image + 1) * columns]
        sums_ref[image : image + 1] = jnp.sum(x, axis=0, keepdims=True)
        sums_ref[images + image : images + image + 1] = jnp.sum(x * x, axis=0, keepdims=True)


def conv(features, sums, gain, bias, level, stale, conv_bias, conv_weight, count):
    cells, channels = features.shape
    return pl.pallas_call(
        functools.partial(conv_body, count=count),
        in_specs=[VMEM] * 8 + [HBM],
        out_specs=[VMEM, VMEM],
        out_shape=[
            jax.ShapeDtypeStruct((cells, channels), F32),
            jax.ShapeDtypeStruct(sums[0].shape, F32),
        ],
        scratch_shapes=[
            pltpu.VMEM(conv_weight.shape[1:], BF16),
            pltpu.SemaphoreType.DMA((1,)),
        ],
        cost_estimate=pl.CostEstimate(
            flops=6 * cells * channels * channels,
            transcendentals=cells * channels,
            bytes_accessed=6 * channels * channels,
        ),
        name="conv",
    )(features, *sums, gain, bias, level, stale, conv_bias, conv_weight)


def attention(queries, key_of, value_of):
    columns, _ = queries.shape
    parts = []
    for first in range(0, HEADS, 4):
        heads = min(4, HEADS - first)
        lanes = slice(first * HEAD_DIM, (first + heads) * HEAD_DIM)
        q = queries[:, lanes]
        lane = lax.broadcasted_iota(jnp.int32, q.shape, 1)
        inside = [(lane >= h * HEAD_DIM) & (lane < (h + 1) * HEAD_DIM) for h in range(heads)]
        stacked = jnp.concatenate([jnp.where(i, q, 0.0) for i in inside], axis=0).astype(BF16)
        scores = lax.dot_general(
            stacked, key_of(lanes), (((1,), (1,)), ((), ())), preferred_element_type=F32
        ) * (HEAD_DIM**-0.5)
        weights = jnp.exp(scores - jnp.max(scores, axis=-1, keepdims=True))
        total = jnp.sum(weights, axis=-1, keepdims=True)
        result = dot(weights.astype(BF16), value_of(lanes)) / total
        part = jnp.zeros_like(q)
        for h in range(heads):
            part = part + jnp.where(inside[h], result[h * columns : (h + 1) * columns], 0.0)
        parts.append(part)
    return jnp.concatenate(parts, axis=-1).astype(BF16)


def tail_body(
    hidden_ref, mine_ref, other_ref, gain_ref, bias_ref, layer_gain_ref, text_keys_ref, text_values_ref,
    near_keys_ref, far_keys_ref, near_values_ref, far_values_ref,
    wq_ref, wk_ref, wv_ref, wo_ref, cq_ref, co_ref,
    out_ref, keys_buf, values_buf, weights_buf, sem, *, count,
):
    near = near_keys_ref.shape[0]
    moves = [
        (wq_ref, weights_buf.at[0]),
        (wk_ref, weights_buf.at[1]),
        (wv_ref, weights_buf.at[2]),
        (near_keys_ref.at[pl.ds(1, near - 1)], keys_buf.at[pl.ds(1, near - 1)]),
        (far_keys_ref, keys_buf.at[pl.ds(near, near)]),
        (near_values_ref.at[pl.ds(1, near - 1)], values_buf.at[pl.ds(1, near - 1)]),
        (far_values_ref, values_buf.at[pl.ds(near, near)]),
        (wo_ref, weights_buf.at[3]),
        (cq_ref, weights_buf.at[4]),
        (co_ref, weights_buf.at[5]),
    ]
    copies = [pltpu.make_async_copy(a, b, sem.at[i]) for i, (a, b) in enumerate(moves)]
    for copy in copies:
        copy.start()
    cells, channels = hidden_ref.shape
    images = text_keys_ref.shape[0]
    columns = cells // images
    patches = 2 * near
    moments = per_channel(mine_ref[...] + other_ref[...], count)
    gain, bias, layer_gain = [r[...].reshape(1, channels) for r in (gain_ref, bias_ref, layer_gain_ref)]
    rows = [slice(image * columns, (image + 1) * columns) for image in range(images)]
    x = jnp.concatenate(
        [
            normalised(hidden_ref[rows[i]], moments, i, images, gain, bias)
            for i in range(images)
        ],
        axis=0,
    ).astype(BF16)
    copies[0].wait()
    queries = dot(x, weights_buf[0]).astype(BF16).astype(F32)
    copies[1].wait()
    keys = dot(x, weights_buf[1]).astype(BF16)
    copies[2].wait()
    values = dot(x, weights_buf[2]).astype(BF16)
    for image in range(images):
        keys_buf[0, image] = keys[rows[image]]
        values_buf[0, image] = values[rows[image]]
    for copy in copies[3:7]:
        copy.wait()
    own = []
    for image in range(images):
        flat = lambda buf, lanes: buf[:, image, :, lanes].reshape(
            patches * columns, lanes.stop - lanes.start
        )
        own.append(
            attention(queries[rows[image]], lambda l: flat(keys_buf, l), lambda l: flat(values_buf, l))
        )
    copies[7].wait()
    mixed = hidden_ref[...] + dot(jnp.concatenate(own, axis=0), weights_buf[3])
    centred = mixed - jnp.mean(mixed, axis=-1, keepdims=True)
    var = jnp.mean(centred * centred, axis=-1, keepdims=True)
    layer_in = (centred * lax.rsqrt(var + EPSILON) * layer_gain).astype(BF16)
    copies[8].wait()
    cross_q = dot(layer_in, weights_buf[4]).astype(BF16).astype(F32)
    crossed = [
        attention(
            cross_q[rows[image]],
            lambda l: text_keys_ref[image, :, l],
            lambda l: text_values_ref[image, :, l],
        )
        for image in range(images)
    ]
    copies[9].wait()
    out_ref[...] = mixed + dot(jnp.concatenate(crossed, axis=0), weights_buf[5])


def tail(hidden, sums, gain, bias, layer_gain, text_keys, text_values, kept, weights, count):
    cells, channels = hidden.shape
    near, images, columns, width = kept[0].shape
    buffer = pltpu.VMEM((2 * near, images, columns, width), BF16)
    return pl.pallas_call(
        functools.partial(tail_body, count=count),
        in_specs=[VMEM] * 8 + [HBM] * 10,
        out_specs=VMEM,
        out_shape=jax.ShapeDtypeStruct((cells, channels), F32),
        scratch_shapes=[
            buffer,
            buffer,
            pltpu.VMEM((6, channels, width), BF16),
            pltpu.SemaphoreType.DMA((10,)),
        ],
        cost_estimate=pl.CostEstimate(
            flops=12 * cells * channels * width + 16 * near * columns * cells * width,
            transcendentals=2 * near * columns * cells * HEADS,
            bytes_accessed=12 * channels * width + 8 * near * images * columns * width,
        ),
        name="tail",
    )(hidden, *sums, gain, bias, layer_gain, text_keys, text_values, *kept, *weights)


def on_device(
    features, stale_conv_in, stale_normed, first_gain, first_bias, conv_weight, conv_bias,
    second_gain, second_bias, query_weight, key_weight, value_weight, output_weight,
    layer_gain, cross_query, cross_output, text_keys, text_values,
):
    images, _, columns, channels = features.shape
    cells = images * columns
    patches = lax.axis_size("patch")
    count = patches * columns * (channels // GROUPS)
    wide = features.astype(F32)[:, 0]
    sums = jnp.concatenate([jnp.sum(wide, axis=1), jnp.sum(wide * wide, axis=1)], axis=0)
    sums = total_over(sums, "patch")

    stale = stale_conv_in[:, 0]
    right_side = lax.axis_index("patch") % 2 == 1
    across = exchange(stale, "patch", 1)
    left = jnp.where(right_side, across[:, -1:], 0)
    right = jnp.where(right_side, 0, across[:, :1])
    level = jnp.concatenate([stale, left, right, jnp.zeros_like(stale[:, :6])], axis=1)
    above = shifted(level, "patch", 2)
    below = shifted(level, "patch", -2)

    held = stale_normed.reshape(1, images, columns, channels)
    apart = patches // 2
    while apart:
        other = exchange(held, "patch", apart)
        if apart > 1:
            held = jnp.concatenate([held, other], axis=0)
        apart //= 2
    kept = []
    for weight in (key_weight, value_weight):
        for part in (held, other):
            kept.append(dot(part.reshape(-1, channels), weight).astype(BF16).reshape(part.shape))

    partial = stale_conv(above, below, conv_weight, cells)
    hidden, sums = conv(
        features.reshape(cells, channels), sums, first_gain, first_bias,
        level, partial, conv_bias, conv_weight, count,
    )
    sums = total_over(sums, "patch")
    out = tail(
        hidden, sums, second_gain, second_bias, layer_gain, text_keys, text_values,
        kept, (query_weight, key_weight, value_weight, output_weight, cross_query, cross_output), count,
    )
    return out.reshape(images, 1, columns, channels)


def solution(mesh):
    split = P("grp", "patch", None, None)
    in_specs = (split,) * 3 + (P(),) * 13 + (P("grp", None, None),) * 2
    return jax.shard_map(on_device, mesh=mesh, in_specs=in_specs, out_specs=split, check_vma=False)
```
